256 devices in a mesh: row: 8 (over z), col: 32 (over x, y, core).
Axes of the slice: x: 4, y: 4, z: 8, core: 2. Of those that a mesh axis runs over, the one named last changes fastest.
Arguments:
- tile_values: bfloat16 [8, 32, 128, 128, 128], P('row', 'col'), may hold values from -0.1875 to 0.1875
- tile_rows: int32 [8, 32, 128], P('row', 'col'), may hold values from 0 to 15, as said below
- tile_cols: int32 [8, 32, 128], P('row', 'col'), may hold values from 0 to 15, as said below
- tile_count: int32 [8, 32], P('row', 'col'), may hold values from 42 to 128, as said below
- sinogram: float32 [16384, 128], P('row'), may hold values from -6 to 6
Outputs:
- solution: float32 [65536, 128], P('col')
- residual_estimate: float32 [128], replicated
The draws below stay inside these ranges and needn't reach their ends.
Inputs may be any that keep to these rules, and one draw needn't show every extreme that they name: On each device the 128 slots name distinct tile positions (tile_rows, tile_cols) of its grid of 16 x 16 tiles. `tile_cols`: see tile_rows. `tile_count`: some device holds 128 tiles in every draw.
All inputs are finite; a program needn't handle non-finite values.
Results may differ from the reference program's by a relative error of at most 0.0019.
Values may be sent and summed in bfloat16 or wider, within the bound.
No kernel may reach another device: no remote copies, remote signals or barrier semaphores. Data moves between devices by JAX's collectives and lax.ppermute only.
A program may use at most 128 MiB of HBM per device.

```python
import jax
import jax.numpy as jnp
from jax import lax

TILE = 128
TR = 16
TC = 16
CAP = 128
Z = 128
ITERS = 3
M = 16384
N_ROW = 8
N_COL = 32


def occupancy(key):
    base = jax.random.fold_in(key, 7)
    device_keys = jax.random.split(base, N_ROW * N_COL)
    orders = jax.vmap(lambda single: jax.random.permutation(single, TR * TC))(device_keys)
    return orders[:, :CAP].reshape(N_ROW, N_COL, CAP).astype(jnp.int32)


def draw_tile_rows(key, part):
    return (occupancy(key) // TC).astype(jnp.int32)


def draw_tile_cols(key, part):
    return (occupancy(key) % TC).astype(jnp.int32)


def draw_tile_count(key, part):
    counts = jax.random.randint(jax.random.fold_in(key, 11), (N_ROW * N_COL,), CAP // 3, CAP + 1)
    fullest = jax.random.randint(jax.random.fold_in(key, 13), (), 0, N_ROW * N_COL)
    flat = jnp.where(jnp.arange(N_ROW * N_COL) == fullest, CAP, counts)
    return flat.reshape(N_ROW, N_COL).astype(jnp.int32)


def steps_of(stream_key, shape, pieces, least, top_value):
    factor_of = 1.0
    for position, parts in pieces:
        steps = jax.random.uniform(jax.random.fold_in(jax.random.fold_in(stream_key, 6), position), (parts,), jnp.float32, least / len(pieces), top_value / len(pieces))
        factor_of = factor_of * jnp.repeat(jnp.exp(steps), shape[position] // parts).reshape((-1,) + (1,) * (len(shape) - 1 - position))
    return factor_of


def scatter_about(stream_key, extent, scale, limit, cuts=(), kind=jnp.bfloat16):
    entries = scale * jax.random.normal(stream_key, extent, jnp.float32)
    if cuts:
        entries = entries * steps_of(stream_key, extent, cuts, -0.22, 0.18)
    return jnp.clip(entries, -limit, limit).astype(kind)


def setup_inputs(seed: int = 0) -> dict:
    arg_keys = jax.random.split(jax.random.key(seed), 6)
    return {
        "tile_values": scatter_about(arg_keys[0], (N_ROW, N_COL, CAP, TILE, TILE), (TILE * CAP // TR) ** -0.5, 0.1875, ((0, 8), (1, 32))),
        "tile_rows": draw_tile_rows(jax.random.fold_in(arg_keys[5], 71), 0),
        "tile_cols": draw_tile_cols(jax.random.fold_in(arg_keys[5], 71), 0),
        "tile_count": draw_tile_count(jax.random.fold_in(arg_keys[5], 71), 0),
        "sinogram": scatter_about(arg_keys[4], (M, Z), 1.0, 6.0, ((0, 8),), jnp.float32),
    }


EPSILON = 1e-06

def column_norm(vec):
    return jnp.sqrt(lax.optimization_barrier(jnp.sum(vec * vec, axis=0)) + EPSILON)

def project(tile_values, tile_rows, tile_cols, tile_count, source, forward):
    operand = source.astype(jnp.bfloat16).astype(jnp.float32)
    slot_ids = jnp.arange(CAP, dtype=jnp.int32)
    if forward:
        out_rows = TR * TILE * N_ROW
        out_blocks = TR
        in_len = TC * TILE
        pattern = 'tij,tjz->tiz'
    else:
        out_rows = TC * TILE * N_COL
        out_blocks = TC
        in_len = TR * TILE
        pattern = 'tji,tjz->tiz'

    def one_device(carry, device_idx):
        row_idx = device_idx // N_COL
        col_idx = device_idx % N_COL
        values = tile_values[row_idx, col_idx].astype(jnp.float32)
        if forward:
            take_index = tile_cols[row_idx, col_idx]
            put_index = tile_rows[row_idx, col_idx]
            in_first = (col_idx * in_len).astype(jnp.int32)
            out_first = (row_idx * (out_blocks * TILE)).astype(jnp.int32)
        else:
            take_index = tile_rows[row_idx, col_idx]
            put_index = tile_cols[row_idx, col_idx]
            in_first = (row_idx * in_len).astype(jnp.int32)
            out_first = (col_idx * (out_blocks * TILE)).astype(jnp.int32)
        blocks = lax.dynamic_slice_in_dim(operand, in_first, in_len, 0).reshape(in_len // TILE, TILE, Z)
        products = jnp.einsum(pattern, values, blocks[take_index], precision=lax.Precision.HIGHEST)
        live_mask = (slot_ids < tile_count[row_idx, col_idx]).astype(jnp.float32)
        targets = jnp.arange(out_blocks, dtype=jnp.int32)
        onehot = (put_index[None, :] == targets[:, None]).astype(jnp.float32) * live_mask[None, :]
        part_sum = jnp.einsum('rt,tiz->riz', onehot, products, precision=lax.Precision.HIGHEST)
        part_sum = part_sum.reshape(out_blocks * TILE, Z)
        current = lax.dynamic_slice_in_dim(carry, out_first, out_blocks * TILE, 0)
        return (lax.dynamic_update_slice_in_dim(carry, current + part_sum, out_first, 0), None)
    start = jnp.zeros((out_rows, Z), jnp.float32)
    result, unused = lax.scan(one_device, start, jnp.arange(N_ROW * N_COL, dtype=jnp.int32))
    return result

def rotation(rho_bar, beta_norm, phi_bar):
    rho_value = jnp.sqrt(rho_bar * rho_bar + beta_norm * beta_norm)
    cosine = rho_bar / rho_value
    sine_value = beta_norm / rho_value
    return (rho_value, cosine, sine_value, cosine * phi_bar, sine_value * phi_bar)

def reference(tile_values, tile_rows, tile_cols, tile_count, sinogram):
    beta_norm = column_norm(sinogram)
    ray_vec = sinogram / beta_norm
    voxel_raw = project(tile_values, tile_rows, tile_cols, tile_count, sinogram, False) / beta_norm
    alpha_norm = column_norm(voxel_raw)
    voxel_vec = voxel_raw / alpha_norm
    search_dir = voxel_vec
    solution = jnp.zeros_like(voxel_vec)
    phi_bar = beta_norm
    rho_bar = alpha_norm
    for step_idx in range(ITERS):
        ray_raw = project(tile_values, tile_rows, tile_cols, tile_count, voxel_raw, True) / alpha_norm - alpha_norm * ray_vec
        beta_norm = column_norm(ray_raw)
        ray_vec = ray_raw / beta_norm
        rho_value, cosine, sine_value, phi_value, phi_bar = rotation(rho_bar, beta_norm, phi_bar)
        solution = solution + phi_value / rho_value * search_dir
        if step_idx + 1 < ITERS:
            voxel_raw = project(tile_values, tile_rows, tile_cols, tile_count, ray_raw, False) / beta_norm - beta_norm * voxel_vec
            alpha_norm = column_norm(voxel_raw)
            voxel_vec = voxel_raw / alpha_norm
            theta_value = sine_value * alpha_norm
            rho_bar = -cosine * alpha_norm
            search_dir = voxel_vec - theta_value / rho_value * search_dir
    return (solution, phi_bar)
```

```python
import jax
import jax.numpy as jnp
from jax import lax
from jax.experimental import pallas as pl
from jax.experimental.pallas import tpu as pltpu
from jax.sharding import Mesh
from jax.sharding import PartitionSpec as P

TILE = 128
ITERS = 3
EPSILON = 1e-06
XY = ("col_0", "col_1")
COL = ("col_0", "col_1", "col_2")
ALL = ("row", "col_0", "col_1", "col_2")
STEPS = 32440.0
META = 8

f32 = jnp.float32
bf16 = jnp.bfloat16
i16 = jnp.int16


def exponent_of(largest):
    return jnp.ceil(jnp.log2(jnp.maximum(largest, 1e-30)))


def coded(array, exponent):
    return jnp.round(array * (jnp.exp2(-exponent) * STEPS)).astype(i16)


def step_of(exponent):
    return jnp.exp2(exponent) * (1.0 / STEPS)


def meta_rows(exponent, squares):
    power = exponent_of(squares)
    scaled = squares * jnp.exp2(-power) * 16384.0
    first = jnp.floor(scaled)
    second = jnp.round((scaled - first) * 16384.0)
    blank = jnp.zeros((META - 4, squares.shape[1]), f32)
    return jnp.concatenate([exponent, power, first, second, blank], axis=0).astype(i16)


def squares_in(meta):
    return jnp.exp2(meta[1:2]) * (meta[2:3] + meta[3:4] * (1.0 / 16384.0)) * (1.0 / 16384.0)


def three_pieces(squares):
    high = squares.astype(bf16)
    rest = squares - high.astype(f32)
    middle = rest.astype(bf16)
    low = (rest - middle.astype(f32)).astype(bf16)
    blank = jnp.zeros((META - 3, squares.shape[1]), f32)
    return jnp.concatenate(
        [high.astype(f32), middle.astype(f32), low.astype(f32), blank], axis=0
    ).astype(bf16)


def column_squares(array):
    return jnp.sum(array * array, axis=0, keepdims=True)


def back_project(matrix_ref, rays, part_ref, out_ref, squares):
    voxels = matrix_ref.shape[1]
    rays_t = rays.astype(f32).T.astype(bf16)
    width = 256
    for first in range(0, voxels, width):
        part = jnp.dot(rays_t, matrix_ref[:, first : first + width], preferred_element_type=f32)
        part_ref[first : first + width, :] = part.T
    part = part_ref[...]
    exponent = exponent_of(jnp.max(jnp.abs(part), axis=0, keepdims=True))
    meta = meta_rows(exponent, squares)
    peers = out_ref.shape[0]
    rows = voxels // peers
    codes = coded(part, exponent)
    for peer in range(peers):
        out_ref[peer, :rows, :] = codes[peer * rows : (peer + 1) * rows]
        out_ref[peer, rows : rows + META, :] = meta


def first_kernel(rows_ref, cols_ref, count_ref, tiles_ref, sinogram_ref, matrix_ref, out_ref, part_ref):
    matrix_ref[...] = jnp.zeros(matrix_ref.shape, bf16)

    def place(slot, carry):
        row = pl.multiple_of(rows_ref[slot] * TILE, TILE)
        col = pl.multiple_of(cols_ref[slot] * TILE, TILE)
        matrix_ref[pl.ds(row, TILE), pl.ds(col, TILE)] = tiles_ref[slot]
        return carry

    lax.fori_loop(0, count_ref[0], place, 0)
    sinogram = sinogram_ref[...]
    back_project(matrix_ref, sinogram.astype(bf16), part_ref, out_ref, column_squares(sinogram))


def backward_kernel(core_ref, matrix_ref, own_ref, other_ref, out_ref, rays_ref, part_ref):
    peers = own_ref.shape[0]
    share = own_ref.shape[1] - META
    core = core_ref[0]
    for source_ref, which in ((own_ref, core), (other_ref, 1 - core)):
        for peer in range(peers):
            start = pl.multiple_of(which * (peers * share) + peer * share, share)
            rays_ref[pl.ds(start, share), :] = source_ref[peer, :share, :]

    def pieces(ref):
        total = jnp.zeros((1, ref.shape[2]), f32)
        for peer in range(peers):
            meta = ref[peer, share : share + META, :].astype(f32)
            total = total + (meta[0:1] + meta[1:2] + meta[2:3])
        return total

    squares = pieces(own_ref) + pieces(other_ref)
    back_project(matrix_ref, rays_ref[...], part_ref, out_ref, squares)


def voxel_kernel(*refs, first):
    if first:
        part_ref, out_ref, raw_ref, beta_ref = refs
    else:
        part_ref, raw_before_ref, alpha_ref, out_ref, raw_ref, beta_ref = refs
    peers = part_ref.shape[0]
    rows = part_ref.shape[1] - META
    total = jnp.zeros((rows, part_ref.shape[2]), f32)
    squares = jnp.zeros((1, part_ref.shape[2]), f32)
    for peer in range(peers):
        meta = part_ref[peer, rows : rows + META, :].astype(f32)
        total = total + part_ref[peer, :rows, :].astype(f32) * step_of(meta[0:1])
        squares = squares + squares_in(meta)
    beta = jnp.sqrt(squares + EPSILON)
    raw = total / beta
    if not first:
        raw = raw - beta * (raw_before_ref[...] / alpha_ref[...])
    exponent = exponent_of(jnp.max(jnp.abs(raw), axis=0, keepdims=True))
    codes = coded(raw, exponent)
    meta = meta_rows(exponent, column_squares(raw))
    for peer in range(peers):
        out_ref[peer, :rows, :] = codes
        out_ref[peer, rows : rows + META, :] = meta
    raw_ref[...] = raw
    beta_ref[...] = beta


def forward_kernel(core_ref, matrix_ref, voxels_ref, own_ref, other_ref, squares_ref, operand_ref, part_ref):
    peers = voxels_ref.shape[0]
    rows = voxels_ref.shape[1] - META
    squares = jnp.zeros((1, voxels_ref.shape[2]), f32)
    for peer in range(peers):
        meta = voxels_ref[peer, rows : rows + META, :].astype(f32)
        voxels = voxels_ref[peer, :rows, :].astype(f32) * step_of(meta[0:1])
        operand_ref[peer * rows : (peer + 1) * rows, :] = voxels.astype(bf16)
        squares = squares + squares_in(meta)
    height = 256
    for first in range(0, matrix_ref.shape[0], height):
        part_ref[first : first + height, :] = jnp.dot(
            matrix_ref[first : first + height, :], operand_ref[...], preferred_element_type=f32
        )
    core = core_ref[0]
    half = own_ref.shape[0]
    own_ref[...] = part_ref[pl.ds(pl.multiple_of(core * half, half), half), :]
    other = part_ref[pl.ds(pl.multiple_of((1 - core) * half, half), half), :]
    exponent = exponent_of(jnp.max(jnp.abs(other), axis=0, keepdims=True))
    meta = meta_rows(exponent, squares)
    other_ref[:half, :] = coded(other, exponent)
    other_ref[half : half + META, :] = meta
    squares_ref[...] = squares_in(meta.astype(f32))


def pair_kernel(own_ref, squares_ref, received_ref, out_ref):
    half = own_ref.shape[0]
    peers = out_ref.shape[0]
    share = half // peers
    meta = received_ref[half : half + META, :].astype(f32)
    part = own_ref[...] + received_ref[:half, :].astype(f32) * step_of(meta[0:1])
    squares = squares_ref[...] + squares_in(meta)
    exponent = exponent_of(jnp.max(jnp.abs(part), axis=0, keepdims=True))
    codes = coded(part, exponent)
    meta = meta_rows(exponent, squares)
    for peer in range(peers):
        out_ref[peer, :share, :] = codes[peer * share : (peer + 1) * share]
        out_ref[peer, share : share + META, :] = meta


def ray_kernel(part_ref, ray_before_ref, beta_ref, *out_refs, last):
    peers = part_ref.shape[0]
    share = part_ref.shape[1] - META
    total = jnp.zeros((share, part_ref.shape[2]), f32)
    squares = jnp.zeros((1, part_ref.shape[2]), f32)
    for peer in range(peers):
        meta = part_ref[peer, share : share + META, :].astype(f32)
        total = total + part_ref[peer, :share, :].astype(f32) * step_of(meta[0:1])
        squares = squares + squares_in(meta)
    alpha = jnp.sqrt(squares + EPSILON)
    raw = total / alpha - alpha * (ray_before_ref[...] / beta_ref[...])
    if last:
        squares_ref, alpha_ref = out_refs
        squares_ref[...] = column_squares(raw)
    else:
        out_ref, raw_ref, alpha_ref = out_refs
        pieces = three_pieces(column_squares(raw))
        rounded = raw.astype(bf16)
        for peer in range(peers):
            out_ref[peer, :share, :] = rounded
            out_ref[peer, share : share + META, :] = pieces
        raw_ref[...] = raw
    alpha_ref[...] = alpha


def rotation(rho_bar, beta_norm, phi_bar):
    rho_value = jnp.sqrt(rho_bar * rho_bar + beta_norm * beta_norm)
    cosine = rho_bar / rho_value
    sine_value = beta_norm / rho_value
    return (rho_value, cosine, sine_value, cosine * phi_bar, sine_value * phi_bar)


def last_kernel(voxels0, voxels1, voxels2, alpha0, alpha1, alpha2, beta0, beta1, beta2, beta3, out_ref, phi_ref):
    voxels = (voxels0, voxels1, voxels2)
    alphas = [ref[...] for ref in (alpha0, alpha1, alpha2)]
    betas = [ref[...] for ref in (beta0, beta1, beta2, beta3)]
    phi_bar = betas[0]
    rho_bar = alphas[0]
    steps, turns = [], []
    for step in range(ITERS):
        rho_value, cosine, sine_value, phi_value, phi_bar = rotation(rho_bar, betas[step + 1], phi_bar)
        steps.append(phi_value / rho_value)
        if step + 1 < ITERS:
            turns.append(sine_value * alphas[step + 1] / rho_value)
            rho_bar = -cosine * alphas[step + 1]
    peers = voxels0.shape[0]
    rows = voxels0.shape[1] - META
    for peer in range(peers):
        solution_rows = search_dir = None
        for step in range(ITERS):
            meta = voxels[step][peer, rows : rows + META, :].astype(f32)
            raw = voxels[step][peer, :rows, :].astype(f32) * step_of(meta[0:1])
            voxel_vec = raw / alphas[step]
            if step == 0:
                search_dir = voxel_vec
                solution_rows = steps[0] * search_dir
            else:
                search_dir = voxel_vec - turns[step - 1] * search_dir
                solution_rows = solution_rows + steps[step] * search_dir
        out_ref[peer * rows : (peer + 1) * rows, :] = solution_rows
    phi_ref[...] = phi_bar


def whole(memory=pltpu.VMEM):
    return pl.BlockSpec(memory_space=memory)


def call(kernel, operands, outs, scratch=(), scalars=0, limit=24):
    shapes = [jax.ShapeDtypeStruct(shape, dtype) for shape, dtype in outs]
    return pl.pallas_call(
        kernel,
        in_specs=[whole(pltpu.SMEM)] * scalars + [whole()] * (len(operands) - scalars),
        out_specs=[whole()] * len(outs),
        out_shape=shapes,
        scratch_shapes=[pltpu.VMEM(shape, dtype) for shape, dtype in scratch],
        compiler_params=pltpu.CompilerParams(vmem_limit_bytes=limit * 1024 * 1024),
    )(*operands)


def exchanged(array, axis):
    return lax.all_to_all(array, axis, 0, 0, tiled=True)


def body(tile_values, tile_rows, tile_cols, tile_count, sinogram):
    rays, depth = sinogram.shape
    peers_row = lax.axis_size("row")
    peers_xy = lax.axis_size(XY)
    voxels = rays
    rows = voxels // peers_row
    half = rays // 2
    share = half // peers_xy
    core = lax.axis_index("col_2")
    core_arg = core.astype(jnp.int32).reshape(1)

    def swapped(array):
        return lax.ppermute(array, "col_2", [(0, 1), (1, 0)])

    row_block = ((peers_row, rows + META, depth), i16)
    norm_row = ((1, depth), f32)
    part = ((rays, depth), f32)

    matrix, sent = call(
        first_kernel,
        (tile_rows[0, 0], tile_cols[0, 0], tile_count[0], tile_values[0, 0], sinogram),
        [((rays, voxels), bf16), row_block],
        [part],
        scalars=3,
        limit=40,
    )
    ray_raw = lax.dynamic_slice_in_dim(sinogram, core * half + lax.axis_index(XY) * share, share, 0)
    voxel_raw = None
    alphas, betas, gathered = [], [], []
    for step in range(ITERS):
        received = exchanged(sent, "row")
        before = () if step == 0 else (voxel_raw, alphas[-1])
        copies, voxel_raw, beta = call(
            lambda *refs, first=step == 0: voxel_kernel(*refs, first=first),
            (received, *before),
            [row_block, ((rows, depth), f32), norm_row],
        )
        betas.append(beta)
        gathered.append(exchanged(copies, "row"))
        own, other, squares = call(
            forward_kernel,
            (core_arg, matrix, gathered[-1]),
            [((half, depth), f32), ((half + META, depth), i16), norm_row],
            [((voxels, depth), bf16), part],
            scalars=1,
        )
        (sent,) = call(
            pair_kernel, (own, squares, swapped(other)), [((peers_xy, share + META, depth), i16)]
        )
        received = exchanged(sent, XY)
        last = step + 1 == ITERS
        outs = [norm_row, norm_row]
        if not last:
            outs = [((peers_xy, share + META, depth), bf16), ((share, depth), f32), norm_row]
        results = call(
            lambda *refs, last=last: ray_kernel(*refs, last=last), (received, ray_raw, beta), outs
        )
        alphas.append(results[-1])
        if not last:
            copies, ray_raw = results[:2]
            own_rays = exchanged(copies, XY)
            (sent,) = call(
                backward_kernel,
                (core_arg, matrix, own_rays, swapped(own_rays)),
                [row_block],
                [((rays, depth), bf16), part],
                scalars=1,
            )
    devices = lax.axis_size(ALL)
    squares = exchanged(jnp.broadcast_to(results[0][None], (devices, 1, depth)), ALL)
    betas.append(jnp.sqrt(jnp.sum(squares, axis=0) + EPSILON))
    answer, phi_bar = call(
        last_kernel, (*gathered, *alphas, *betas), [((voxels, depth), f32), norm_row]
    )
    return answer, phi_bar[0]


def solution(mesh):
    split = Mesh(mesh.devices.reshape(mesh.shape["row"], 4, 4, 2), ("row", *COL))
    placed = (
        P("row", COL, None, None, None),
        P("row", COL, None),
        P("row", COL, None),
        P("row", COL),
        P("row", None),
    )
    return jax.shard_map(
        body, mesh=split, in_specs=placed, out_specs=(P(COL, None), P()), check_vma=False
    )
```

```python
import jax
import jax.numpy as jnp
from jax import lax
from jax.experimental import pallas as pl
from jax.experimental.pallas import tpu as pltpu
from jax.sharding import Mesh
from jax.sharding import PartitionSpec as P

TILE = 128
ITERS = 3
EPSILON = 1e-06
XY = ("col_0", "col_1")
COL = ("col_0", "col_1", "col_2")
ALL = ("row", "col_0", "col_1", "col_2")
STEPS = 32440.0
META = 8
STAGGER = 7000

f32 = jnp.float32
bf16 = jnp.bfloat16
i16 = jnp.int16


def exponent_of(largest):
    return jnp.ceil(jnp.log2(jnp.maximum(largest, 1e-30)))


def coded(array, exponent):
    return jnp.round(array * (jnp.exp2(-exponent) * STEPS)).astype(i16)


def step_of(exponent):
    return jnp.exp2(exponent) * (1.0 / STEPS)


def meta_rows(exponent, squares):
    power = exponent_of(squares)
    scaled = squares * jnp.exp2(-power) * 16384.0
    first = jnp.floor(scaled)
    second = jnp.round((scaled - first) * 16384.0)
    blank = jnp.zeros((META - 4, squares.shape[1]), f32)
    return jnp.concatenate([exponent, power, first, second, blank], axis=0).astype(i16)


def squares_in(meta):
    return jnp.exp2(meta[1:2]) * (meta[2:3] + meta[3:4] * (1.0 / 16384.0)) * (1.0 / 16384.0)


def three_pieces(squares):
    high = squares.astype(bf16)
    rest = squares - high.astype(f32)
    middle = rest.astype(bf16)
    low = (rest - middle.astype(f32)).astype(bf16)
    blank = jnp.zeros((META - 3, squares.shape[1]), f32)
    return jnp.concatenate(
        [high.astype(f32), middle.astype(f32), low.astype(f32), blank], axis=0
    ).astype(bf16)


def column_squares(array):
    return jnp.sum(array * array, axis=0, keepdims=True)


def back_project(matrix_ref, rays, part_ref, out_ref, squares):
    voxels = matrix_ref.shape[1]
    rays_t = rays.astype(f32).T.astype(bf16)
    width = 256
    for first in range(0, voxels, width):
        part = jnp.dot(rays_t, matrix_ref[:, first : first + width], preferred_element_type=f32)
        part_ref[first : first + width, :] = part.T
    part = part_ref[...]
    exponent = exponent_of(jnp.max(jnp.abs(part), axis=0, keepdims=True))
    meta = meta_rows(exponent, squares)
    peers = out_ref.shape[0]
    rows = voxels // peers
    codes = coded(part, exponent)
    for peer in range(peers):
        out_ref[peer, :rows, :] = codes[peer * rows : (peer + 1) * rows]
        out_ref[peer, rows : rows + META, :] = meta


def first_kernel(
    start_ref, count_ref, rows_ref, cols_ref, tiles_ref, sinogram_ref,
    matrix_ref, out_ref, share_ref,
    rows_here, cols_here, sinogram_here, part_ref, small_sems, tile_sems,
):
    copies = [
        pltpu.make_async_copy(rows_ref.at[0, 0], rows_here, small_sems.at[0]),
        pltpu.make_async_copy(cols_ref.at[0, 0], cols_here, small_sems.at[1]),
        pltpu.make_async_copy(sinogram_ref, sinogram_here, small_sems.at[2]),
    ]
    for copy in copies:
        copy.start()
    matrix_ref[...] = jnp.zeros(matrix_ref.shape, bf16)
    copies[0].wait()
    copies[1].wait()
    count = count_ref[0]

    def tile_copy(slot):
        row = pl.multiple_of(rows_here[slot] * TILE, TILE)
        col = pl.multiple_of(cols_here[slot] * TILE, TILE)
        target = matrix_ref.at[pl.ds(row, TILE), pl.ds(col, TILE)]
        return pltpu.make_async_copy(tiles_ref.at[0, 0, slot], target, tile_sems.at[slot])

    def begin(slot, carry):
        tile_copy(slot).start()
        return carry

    def finish(slot, carry):
        tile_copy(slot).wait()
        return carry

    lax.fori_loop(0, count, begin, 0)
    copies[2].wait()
    sinogram = sinogram_here[...]
    squares = column_squares(sinogram)
    share = share_ref.shape[0]
    share_ref[...] = sinogram_here[pl.ds(pl.multiple_of(start_ref[0], share), share), :]
    lax.fori_loop(0, count, finish, 0)
    back_project(matrix_ref, sinogram.astype(bf16), part_ref, out_ref, squares)

    @pl.when(start_ref[0] >= sinogram.shape[0] // 2)
    def _():
        pl.delay(STAGGER)


def backward_kernel(core_ref, matrix_ref, own_ref, other_ref, out_ref, rays_ref, part_ref):
    peers = own_ref.shape[0]
    share = own_ref.shape[1] - META
    core = core_ref[0]
    for source_ref, which in ((own_ref, core), (other_ref, 1 - core)):
        for peer in range(peers):
            start = pl.multiple_of(which * (peers * share) + peer * share, share)
            rays_ref[pl.ds(start, share), :] = source_ref[peer, :share, :]

    def pieces(ref):
        total = jnp.zeros((1, ref.shape[2]), f32)
        for peer in range(peers):
            meta = ref[peer, share : share + META, :].astype(f32)
            total = total + (meta[0:1] + meta[1:2] + meta[2:3])
        return total

    squares = pieces(own_ref) + pieces(other_ref)
    back_project(matrix_ref, rays_ref[...], part_ref, out_ref, squares)

    @pl.when(core_ref[0] == 1)
    def _():
        pl.delay(STAGGER)


def voxel_kernel(*refs, first):
    if first:
        part_ref, out_ref, beta_ref, *raw_refs = refs
    else:
        part_ref, raw_before_ref, alpha_ref, out_ref, beta_ref, *raw_refs = refs
    peers = part_ref.shape[0]
    rows = part_ref.shape[1] - META
    total = jnp.zeros((rows, part_ref.shape[2]), f32)
    squares = jnp.zeros((1, part_ref.shape[2]), f32)
    for peer in range(peers):
        meta = part_ref[peer, rows : rows + META, :].astype(f32)
        total = total + part_ref[peer, :rows, :].astype(f32) * step_of(meta[0:1])
        squares = squares + squares_in(meta)
    beta = jnp.sqrt(squares + EPSILON)
    raw = total / beta
    if not first:
        raw = raw - beta * (raw_before_ref[...] / alpha_ref[...])
    exponent = exponent_of(jnp.max(jnp.abs(raw), axis=0, keepdims=True))
    codes = coded(raw, exponent)
    meta = meta_rows(exponent, column_squares(raw))
    for peer in range(peers):
        out_ref[peer, :rows, :] = codes
        out_ref[peer, rows : rows + META, :] = meta
    for raw_ref in raw_refs:
        raw_ref[...] = raw
    beta_ref[...] = beta


def dense_rows(matrix_ref, start, operand_ref, put):
    height = 256
    for first in range(0, matrix_ref.shape[0] // 2, height):
        rows = pl.ds(pl.multiple_of(start + first, height), height)
        put(first, jnp.dot(matrix_ref[rows, :], operand_ref[...], preferred_element_type=f32))


def forward_kernel(core_ref, matrix_ref, voxels_ref, operand_ref, other_ref, squares_ref, part_ref):
    peers = voxels_ref.shape[0]
    rows = voxels_ref.shape[1] - META
    squares = jnp.zeros((1, voxels_ref.shape[2]), f32)
    for peer in range(peers):
        meta = voxels_ref[peer, rows : rows + META, :].astype(f32)
        voxels = voxels_ref[peer, :rows, :].astype(f32) * step_of(meta[0:1])
        operand_ref[peer * rows : (peer + 1) * rows, :] = voxels.astype(bf16)
        squares = squares + squares_in(meta)
    half = part_ref.shape[0]

    def put(first, part):
        part_ref[first : first + part.shape[0], :] = part

    dense_rows(matrix_ref, (1 - core_ref[0]) * half, operand_ref, put)
    other = part_ref[...]
    exponent = exponent_of(jnp.max(jnp.abs(other), axis=0, keepdims=True))
    meta = meta_rows(exponent, squares)
    other_ref[:half, :] = coded(other, exponent)
    other_ref[half : half + META, :] = meta
    squares_ref[...] = squares_in(meta.astype(f32))


def own_kernel(core_ref, matrix_ref, operand_ref, own_ref):
    def put(first, part):
        own_ref[first : first + part.shape[0], :] = part

    dense_rows(matrix_ref, core_ref[0] * own_ref.shape[0], operand_ref, put)


def pair_kernel(own_ref, squares_ref, received_ref, out_ref):
    half = own_ref.shape[0]
    peers = out_ref.shape[0]
    share = half // peers
    meta = received_ref[half : half + META, :].astype(f32)
    part = own_ref[...] + received_ref[:half, :].astype(f32) * step_of(meta[0:1])
    squares = squares_ref[...] + squares_in(meta)
    exponent = exponent_of(jnp.max(jnp.abs(part), axis=0, keepdims=True))
    codes = coded(part, exponent)
    meta = meta_rows(exponent, squares)
    for peer in range(peers):
        out_ref[peer, :share, :] = codes[peer * share : (peer + 1) * share]
        out_ref[peer, share : share + META, :] = meta


def ray_kernel(part_ref, ray_before_ref, beta_ref, *out_refs, last):
    peers = part_ref.shape[0]
    share = part_ref.shape[1] - META
    total = jnp.zeros((share, part_ref.shape[2]), f32)
    squares = jnp.zeros((1, part_ref.shape[2]), f32)
    for peer in range(peers):
        meta = part_ref[peer, share : share + META, :].astype(f32)
        total = total + part_ref[peer, :share, :].astype(f32) * step_of(meta[0:1])
        squares = squares + squares_in(meta)
    alpha = jnp.sqrt(squares + EPSILON)
    raw = total / alpha - alpha * (ray_before_ref[...] / beta_ref[...])
    if last:
        squares_ref, alpha_ref = out_refs
        squares_ref[...] = column_squares(raw)
    else:
        out_ref, raw_ref, alpha_ref = out_refs
        pieces = three_pieces(column_squares(raw))
        rounded = raw.astype(bf16)
        for peer in range(peers):
            out_ref[peer, :share, :] = rounded
            out_ref[peer, share : share + META, :] = pieces
        raw_ref[...] = raw
    alpha_ref[...] = alpha


def rotation(rho_bar, beta_norm, phi_bar):
    rho_value = jnp.sqrt(rho_bar * rho_bar + beta_norm * beta_norm)
    cosine = rho_bar / rho_value
    sine_value = beta_norm / rho_value
    return (rho_value, cosine, sine_value, cosine * phi_bar, sine_value * phi_bar)


def last_kernel(voxels0, voxels1, voxels2, alpha0, alpha1, alpha2, beta0, beta1, beta2, beta3, out_ref, phi_ref):
    voxels = (voxels0, voxels1, voxels2)
    alphas = [ref[...] for ref in (alpha0, alpha1, alpha2)]
    betas = [ref[...] for ref in (beta0, beta1, beta2, beta3)]
    phi_bar = betas[0]
    rho_bar = alphas[0]
    steps, turns = [], []
    for step in range(ITERS):
        rho_value, cosine, sine_value, phi_value, phi_bar = rotation(rho_bar, betas[step + 1], phi_bar)
        steps.append(phi_value / rho_value)
        if step + 1 < ITERS:
            turns.append(sine_value * alphas[step + 1] / rho_value)
            rho_bar = -cosine * alphas[step + 1]
    peers = voxels0.shape[0]
    rows = voxels0.shape[1] - META
    for peer in range(peers):
        solution_rows = search_dir = None
        for step in range(ITERS):
            meta = voxels[step][peer, rows : rows + META, :].astype(f32)
            raw = voxels[step][peer, :rows, :].astype(f32) * step_of(meta[0:1])
            voxel_vec = raw / alphas[step]
            if step == 0:
                search_dir = voxel_vec
                solution_rows = steps[0] * search_dir
            else:
                search_dir = voxel_vec - turns[step - 1] * search_dir
                solution_rows = solution_rows + steps[step] * search_dir
        out_ref[peer * rows : (peer + 1) * rows, :] = solution_rows
    phi_ref[...] = phi_bar


def whole(memory=pltpu.VMEM):
    return pl.BlockSpec(memory_space=memory)


def call(kernel, operands, outs, scratch=(), scalars=0, limit=8):
    shapes = [jax.ShapeDtypeStruct(shape, dtype) for shape, dtype in outs]
    return pl.pallas_call(
        kernel,
        in_specs=[whole(pltpu.SMEM)] * scalars + [whole()] * (len(operands) - scalars),
        out_specs=[whole()] * len(outs),
        out_shape=shapes,
        scratch_shapes=[pltpu.VMEM(shape, dtype) for shape, dtype in scratch],
        compiler_params=pltpu.CompilerParams(vmem_limit_bytes=limit * 1024 * 1024),
    )(*operands)


def exchanged(array, axis):
    return lax.all_to_all(array, axis, 0, 0, tiled=True)


def body(tile_values, tile_rows, tile_cols, tile_count, sinogram):
    rays, depth = sinogram.shape
    peers_row = lax.axis_size("row")
    peers_xy = lax.axis_size(XY)
    voxels = rays
    rows = voxels // peers_row
    half = rays // 2
    share = half // peers_xy
    core = lax.axis_index("col_2")
    core_arg = core.astype(jnp.int32).reshape(1)

    def swapped(array):
        return lax.ppermute(array, "col_2", [(0, 1), (1, 0)])

    row_block = ((peers_row, rows + META, depth), i16)
    norm_row = ((1, depth), f32)
    part = ((rays, depth), f32)

    start = (core * half + lax.axis_index(XY) * share).astype(jnp.int32).reshape(1)
    slots = tile_rows.shape[-1]
    matrix, sent, ray_raw = pl.pallas_call(
        first_kernel,
        in_specs=[whole(pltpu.SMEM)] * 2 + [whole(pltpu.HBM)] * 4,
        out_specs=[whole()] * 3,
        out_shape=[
            jax.ShapeDtypeStruct((rays, voxels), bf16),
            jax.ShapeDtypeStruct(*row_block),
            jax.ShapeDtypeStruct((share, depth), f32),
        ],
        scratch_shapes=[
            pltpu.SMEM((slots,), jnp.int32),
            pltpu.SMEM((slots,), jnp.int32),
            pltpu.VMEM((rays, depth), f32),
            pltpu.VMEM((rays, depth), f32),
            pltpu.SemaphoreType.DMA((3,)),
            pltpu.SemaphoreType.DMA((slots,)),
        ],
        compiler_params=pltpu.CompilerParams(vmem_limit_bytes=16 * 1024 * 1024),
    )(
        start,
        tile_count[0],
        *(
            pltpu.with_memory_space_constraint(array, pltpu.HBM)
            for array in (tile_rows, tile_cols, tile_values, sinogram)
        ),
    )
    voxel_raw = None
    alphas, betas, gathered = [], [], []
    for step in range(ITERS):
        received = exchanged(sent, "row")
        before = () if step == 0 else (voxel_raw, alphas[-1])
        last = step + 1 == ITERS
        copies, beta, *raw = call(
            lambda *refs, first=step == 0: voxel_kernel(*refs, first=first),
            (received, *before),
            [row_block, norm_row] + [((rows, depth), f32)] * (not last),
        )
        if raw:
            voxel_raw = raw[0]
        betas.append(beta)
        gathered.append(exchanged(copies, "row"))
        operand, other, squares = call(
            forward_kernel,
            (core_arg, matrix, gathered[-1]),
            [((voxels, depth), bf16), ((half + META, depth), i16), norm_row],
            [((half, depth), f32)],
            scalars=1,
        )
        others = swapped(other)
        (own,) = call(own_kernel, (core_arg, matrix, operand), [((half, depth), f32)], scalars=1)
        (sent,) = call(
            pair_kernel, (own, squares, others), [((peers_xy, share + META, depth), i16)]
        )
        received = exchanged(sent, XY)
        outs = [norm_row, norm_row]
        if not last:
            outs = [((peers_xy, share + META, depth), bf16), ((share, depth), f32), norm_row]
        results = call(
            lambda *refs, last=last: ray_kernel(*refs, last=last), (received, ray_raw, beta), outs
        )
        alphas.append(results[-1])
        if not last:
            copies, ray_raw = results[:2]
            own_rays = exchanged(copies, XY)
            (sent,) = call(
                backward_kernel,
                (core_arg, matrix, own_rays, swapped(own_rays)),
                [row_block],
                [((rays, depth), bf16), part],
                scalars=1,
            )
    devices = lax.axis_size(ALL)
    squares = exchanged(jnp.broadcast_to(results[0][None], (devices, 1, depth)), ALL)
    betas.append(jnp.sqrt(jnp.sum(squares, axis=0) + EPSILON))
    answer, phi_bar = call(
        last_kernel, (*gathered, *alphas, *betas), [((voxels, depth), f32), norm_row]
    )
    return answer, phi_bar[0]


def solution(mesh):
    split = Mesh(mesh.devices.reshape(mesh.shape["row"], 4, 4, 2), ("row", *COL))
    placed = (
        P("row", COL, None, None, None),
        P("row", COL, None),
        P("row", COL, None),
        P("row", COL),
        P("row", None),
    )
    return jax.shard_map(
        body, mesh=split, in_specs=placed, out_specs=(P(COL, None), P()), check_vma=False
    )
```

```python
import jax
import jax.numpy as jnp
from jax import lax
from jax.experimental import pallas as pl
from jax.experimental.pallas import tpu as pltpu
from jax.sharding import Mesh
from jax.sharding import PartitionSpec as P

TILE = 128
WIDTH = 256
CHUNKS = 4
ITERS = 3
EPSILON = 1e-06
XY = ("col_0", "col_1")
COL = ("col_0", "col_1", "col_2")
ROW_XY = ("row", "col_0", "col_1")
STEPS = 32440.0
META = 8
STAGGER = 7000

f32 = jnp.float32
bf16 = jnp.bfloat16
i16 = jnp.int16


def exponent_of(largest):
    return jnp.ceil(jnp.log2(jnp.maximum(largest, 1e-30)))


def coded(array, exponent):
    return jnp.round(array * (jnp.exp2(-exponent) * STEPS)).astype(i16)


def step_of(exponent):
    return jnp.exp2(exponent) * (1.0 / STEPS)


def meta_rows(exponent, squares):
    power = exponent_of(squares)
    scaled = squares * jnp.exp2(-power) * 16384.0
    first = jnp.floor(scaled)
    second = jnp.round((scaled - first) * 16384.0)
    blank = jnp.zeros((META - 4, squares.shape[1]), f32)
    return jnp.concatenate([exponent, power, first, second, blank], axis=0).astype(i16)


def squares_in(meta):
    return jnp.exp2(meta[1:2]) * (meta[2:3] + meta[3:4] * (1.0 / 16384.0)) * (1.0 / 16384.0)


def three_pieces(squares):
    high = squares.astype(bf16)
    rest = squares - high.astype(f32)
    middle = rest.astype(bf16)
    low = (rest - middle.astype(f32)).astype(bf16)
    blank = jnp.zeros((META - 3, squares.shape[1]), f32)
    return jnp.concatenate(
        [high.astype(f32), middle.astype(f32), low.astype(f32), blank], axis=0
    ).astype(bf16)


def column_squares(array):
    return jnp.sum(array * array, axis=0, keepdims=True)


def send_parts(part_ref, out_ref, squares):
    part = part_ref[...]
    exponent = exponent_of(jnp.max(jnp.abs(part), axis=0, keepdims=True))
    meta = meta_rows(exponent, squares)
    peers = out_ref.shape[0]
    rows = part.shape[0] // peers
    codes = coded(part, exponent)
    for peer in range(peers):
        out_ref[peer, :rows, :] = codes[peer * rows : (peer + 1) * rows]
        out_ref[peer, rows : rows + META, :] = meta


def transposed(rays):
    return rays.astype(f32).T.astype(bf16)


def first_kernel(
    start_ref, count_ref, rows_ref, cols_ref, tiles_ref, sinogram_ref,
    matrix_ref, out_ref, share_ref,
    rows_here, cols_here, sinogram_here, tiles_here, rays_ref, part_ref, sems,
):
    copies = [
        pltpu.make_async_copy(rows_ref.at[0, 0], rows_here, sems.at[0]),
        pltpu.make_async_copy(cols_ref.at[0, 0], cols_here, sems.at[1]),
        pltpu.make_async_copy(sinogram_ref, sinogram_here, sems.at[2]),
    ]
    chunk = tiles_here.shape[0] // CHUNKS
    for index in range(CHUNKS):
        slots = pl.ds(index * chunk, chunk)
        source = tiles_ref.at[0, 0, slots]
        copies.append(pltpu.make_async_copy(source, tiles_here.at[slots], sems.at[3 + index]))
    for copy in copies:
        copy.start()
    matrix_ref[...] = jnp.zeros(matrix_ref.shape, bf16)
    for copy in copies[:3]:
        copy.wait()
    sinogram = sinogram_here[...]
    squares = column_squares(sinogram)
    rays_ref[...] = transposed(sinogram.astype(bf16))
    share = share_ref.shape[0]
    share_ref[...] = sinogram_here[pl.ds(pl.multiple_of(start_ref[0], share), share), :]

    def place(slot, carry):
        row = pl.multiple_of(rows_here[slot] * TILE, TILE)
        col = pl.multiple_of(cols_here[slot] * TILE, TILE)
        matrix_ref[pl.ds(row, TILE), pl.ds(col, TILE)] = tiles_here[slot]
        return carry

    for index in range(CHUNKS):
        copies[3 + index].wait()
        end = jnp.minimum(count_ref[0], (index + 1) * chunk)
        lax.fori_loop(index * chunk, end, place, 0)
    rays_t = rays_ref[...]
    for first in range(0, matrix_ref.shape[1], WIDTH):
        part = jnp.dot(rays_t, matrix_ref[:, first : first + WIDTH], preferred_element_type=f32)
        part_ref[first : first + WIDTH, :] = part.T
    send_parts(part_ref, out_ref, squares)

    @pl.when(start_ref[0] >= sinogram.shape[0] // 2)
    def _():
        pl.delay(STAGGER)


def half_of_rays(source_ref, rays_ref):
    peers = source_ref.shape[0]
    share = source_ref.shape[1] - META
    squares = jnp.zeros((1, source_ref.shape[2]), f32)
    for peer in range(peers):
        rays_ref[peer * share : (peer + 1) * share, :] = source_ref[peer, :share, :]
        meta = source_ref[peer, share : share + META, :].astype(f32)
        squares = squares + (meta[0:1] + meta[1:2] + meta[2:3])
    return transposed(rays_ref[...]), squares


def half_of_matrix(matrix_ref, which, first):
    half = matrix_ref.shape[0] // 2
    start = pl.multiple_of(which * half, half)
    return matrix_ref[pl.ds(start, half), first : first + WIDTH]


def own_backward_kernel(core_ref, matrix_ref, own_ref, sum_ref, squares_ref, rays_ref):
    rays_t, squares_ref[...] = half_of_rays(own_ref, rays_ref)
    for first in range(0, matrix_ref.shape[1], WIDTH):
        sum_ref[:, first : first + WIDTH] = jnp.dot(
            rays_t, half_of_matrix(matrix_ref, core_ref[0], first), preferred_element_type=f32
        )


def backward_kernel(core_ref, matrix_ref, sum_ref, squares_ref, other_ref, out_ref, rays_ref, part_ref):
    rays_t, squares = half_of_rays(other_ref, rays_ref)
    for first in range(0, matrix_ref.shape[1], WIDTH):
        part = sum_ref[:, first : first + WIDTH] + jnp.dot(
            rays_t, half_of_matrix(matrix_ref, 1 - core_ref[0], first), preferred_element_type=f32
        )
        part_ref[first : first + WIDTH, :] = part.T
    send_parts(part_ref, out_ref, squares_ref[...] + squares)

    @pl.when(core_ref[0] == 1)
    def _():
        pl.delay(STAGGER)


def voxel_kernel(*refs, first):
    if first:
        part_ref, out_ref, beta_ref, *raw_refs = refs
    else:
        part_ref, raw_before_ref, alpha_ref, out_ref, beta_ref, *raw_refs = refs
    peers = part_ref.shape[0]
    rows = part_ref.shape[1] - META
    total = jnp.zeros((rows, part_ref.shape[2]), f32)
    squares = jnp.zeros((1, part_ref.shape[2]), f32)
    for peer in range(peers):
        meta = part_ref[peer, rows : rows + META, :].astype(f32)
        total = total + part_ref[peer, :rows, :].astype(f32) * step_of(meta[0:1])
        squares = squares + squares_in(meta)
    beta = jnp.sqrt(squares + EPSILON)
    raw = total / beta
    if not first:
        raw = raw - beta * (raw_before_ref[...] / alpha_ref[...])
    exponent = exponent_of(jnp.max(jnp.abs(raw), axis=0, keepdims=True))
    codes = coded(raw, exponent)
    meta = meta_rows(exponent, column_squares(raw))
    for peer in range(peers):
        out_ref[peer, :rows, :] = codes
        out_ref[peer, rows : rows + META, :] = meta
    for raw_ref in raw_refs:
        raw_ref[...] = raw
    beta_ref[...] = beta


def dense_rows(matrix_ref, start, operand_ref, put):
    height = 256
    for first in range(0, matrix_ref.shape[0] // 2, height):
        rows = pl.ds(pl.multiple_of(start + first, height), height)
        put(first, jnp.dot(matrix_ref[rows, :], operand_ref[...], preferred_element_type=f32))


def forward_kernel(core_ref, matrix_ref, voxels_ref, operand_ref, other_ref, squares_ref, part_ref):
    peers = voxels_ref.shape[0]
    rows = voxels_ref.shape[1] - META
    squares = jnp.zeros((1, voxels_ref.shape[2]), f32)
    for peer in range(peers):
        meta = voxels_ref[peer, rows : rows + META, :].astype(f32)
        voxels = voxels_ref[peer, :rows, :].astype(f32) * step_of(meta[0:1])
        operand_ref[peer * rows : (peer + 1) * rows, :] = voxels.astype(bf16)
        squares = squares + squares_in(meta)
    half = part_ref.shape[0]

    def put(first, part):
        part_ref[first : first + part.shape[0], :] = part

    dense_rows(matrix_ref, (1 - core_ref[0]) * half, operand_ref, put)
    other = part_ref[...]
    exponent = exponent_of(jnp.max(jnp.abs(other), axis=0, keepdims=True))
    meta = meta_rows(exponent, squares)
    other_ref[:half, :] = coded(other, exponent)
    other_ref[half : half + META, :] = meta
    squares_ref[...] = squares_in(meta.astype(f32))


def own_kernel(core_ref, matrix_ref, operand_ref, own_ref):
    def put(first, part):
        own_ref[first : first + part.shape[0], :] = part

    dense_rows(matrix_ref, core_ref[0] * own_ref.shape[0], operand_ref, put)


def pair_kernel(own_ref, squares_ref, received_ref, out_ref):
    half = own_ref.shape[0]
    peers = out_ref.shape[0]
    share = half // peers
    meta = received_ref[half : half + META, :].astype(f32)
    part = own_ref[...] + received_ref[:half, :].astype(f32) * step_of(meta[0:1])
    squares = squares_ref[...] + squares_in(meta)
    exponent = exponent_of(jnp.max(jnp.abs(part), axis=0, keepdims=True))
    codes = coded(part, exponent)
    meta = meta_rows(exponent, squares)
    for peer in range(peers):
        out_ref[peer, :share, :] = codes[peer * share : (peer + 1) * share]
        out_ref[peer, share : share + META, :] = meta


def ray_kernel(part_ref, ray_before_ref, beta_ref, *out_refs, last):
    peers = part_ref.shape[0]
    share = part_ref.shape[1] - META
    total = jnp.zeros((share, part_ref.shape[2]), f32)
    squares = jnp.zeros((1, part_ref.shape[2]), f32)
    for peer in range(peers):
        meta = part_ref[peer, share : share + META, :].astype(f32)
        total = total + part_ref[peer, :share, :].astype(f32) * step_of(meta[0:1])
        squares = squares + squares_in(meta)
    alpha = jnp.sqrt(squares + EPSILON)
    raw = total / alpha - alpha * (ray_before_ref[...] / beta_ref[...])
    if last:
        squares_ref, alpha_ref = out_refs
        squares_ref[...] = column_squares(raw)
    else:
        out_ref, raw_ref, alpha_ref = out_refs
        pieces = three_pieces(column_squares(raw))
        rounded = raw.astype(bf16)
        for peer in range(peers):
            out_ref[peer, :share, :] = rounded
            out_ref[peer, share : share + META, :] = pieces
        raw_ref[...] = raw
    alpha_ref[...] = alpha


def rotation(rho_bar, beta_norm, phi_bar):
    rho_value = jnp.sqrt(rho_bar * rho_bar + beta_norm * beta_norm)
    cosine = rho_bar / rho_value
    sine_value = beta_norm / rho_value
    return (rho_value, cosine, sine_value, cosine * phi_bar, sine_value * phi_bar)


def last_kernel(voxels0, voxels1, voxels2, alpha0, alpha1, alpha2, beta0, beta1, beta2, beta3, out_ref, phi_ref):
    voxels = (voxels0, voxels1, voxels2)
    alphas = [ref[...] for ref in (alpha0, alpha1, alpha2)]
    betas = [ref[...] for ref in (beta0, beta1, beta2, beta3)]
    phi_bar = betas[0]
    rho_bar = alphas[0]
    steps, turns = [], []
    for step in range(ITERS):
        rho_value, cosine, sine_value, phi_value, phi_bar = rotation(rho_bar, betas[step + 1], phi_bar)
        steps.append(phi_value / rho_value)
        if step + 1 < ITERS:
            turns.append(sine_value * alphas[step + 1] / rho_value)
            rho_bar = -cosine * alphas[step + 1]
    peers = voxels0.shape[0]
    rows = voxels0.shape[1] - META
    for peer in range(peers):
        solution_rows = search_dir = None
        for step in range(ITERS):
            meta = voxels[step][peer, rows : rows + META, :].astype(f32)
            raw = voxels[step][peer, :rows, :].astype(f32) * step_of(meta[0:1])
            voxel_vec = raw / alphas[step]
            if step == 0:
                search_dir = voxel_vec
                solution_rows = steps[0] * search_dir
            else:
                search_dir = voxel_vec - turns[step - 1] * search_dir
                solution_rows = solution_rows + steps[step] * search_dir
        out_ref[peer * rows : (peer + 1) * rows, :] = solution_rows
    phi_ref[...] = phi_bar


def whole(memory=pltpu.VMEM):
    return pl.BlockSpec(memory_space=memory)


def call(kernel, operands, outs, scratch=(), scalars=0, limit=8):
    shapes = [jax.ShapeDtypeStruct(shape, dtype) for shape, dtype in outs]
    return pl.pallas_call(
        kernel,
        in_specs=[whole(pltpu.SMEM)] * scalars + [whole()] * (len(operands) - scalars),
        out_specs=[whole()] * len(outs),
        out_shape=shapes,
        scratch_shapes=[pltpu.VMEM(shape, dtype) for shape, dtype in scratch],
        compiler_params=pltpu.CompilerParams(vmem_limit_bytes=limit * 1024 * 1024),
    )(*operands)


def exchanged(array, axis):
    return lax.all_to_all(array, axis, 0, 0, tiled=True)


def body(tile_values, tile_rows, tile_cols, tile_count, sinogram):
    rays, depth = sinogram.shape
    peers_row = lax.axis_size("row")
    peers_xy = lax.axis_size(XY)
    voxels = rays
    rows = voxels // peers_row
    half = rays // 2
    share = half // peers_xy
    core = lax.axis_index("col_2")
    core_arg = core.astype(jnp.int32).reshape(1)

    def swapped(array):
        return lax.ppermute(array, "col_2", [(0, 1), (1, 0)])

    row_block = ((peers_row, rows + META, depth), i16)
    norm_row = ((1, depth), f32)
    part = ((rays, depth), f32)

    start = (core * half + lax.axis_index(XY) * share).astype(jnp.int32).reshape(1)
    slots = tile_rows.shape[-1]
    matrix, sent, ray_raw = pl.pallas_call(
        first_kernel,
        in_specs=[whole(pltpu.SMEM)] * 2 + [whole(pltpu.HBM)] * 4,
        out_specs=[whole()] * 3,
        out_shape=[
            jax.ShapeDtypeStruct((rays, voxels), bf16),
            jax.ShapeDtypeStruct(*row_block),
            jax.ShapeDtypeStruct((share, depth), f32),
        ],
        scratch_shapes=[
            pltpu.SMEM((slots,), jnp.int32),
            pltpu.SMEM((slots,), jnp.int32),
            pltpu.VMEM((rays, depth), f32),
            pltpu.VMEM(tile_values.shape[2:], bf16),
            pltpu.VMEM((depth, rays), bf16),
            pltpu.VMEM((rays, depth), f32),
            pltpu.SemaphoreType.DMA((3 + CHUNKS,)),
        ],
        compiler_params=pltpu.CompilerParams(vmem_limit_bytes=16 * 1024 * 1024),
    )(
        start,
        tile_count[0],
        *(
            pltpu.with_memory_space_constraint(array, pltpu.HBM)
            for array in (tile_rows, tile_cols, tile_values, sinogram)
        ),
    )
    voxel_raw = None
    alphas, betas, gathered = [], [], []
    for step in range(ITERS):
        received = exchanged(sent, "row")
        before = () if step == 0 else (voxel_raw, alphas[-1])
        last = step + 1 == ITERS
        copies, beta, *raw = call(
            lambda *refs, first=step == 0: voxel_kernel(*refs, first=first),
            (received, *before),
            [row_block, norm_row] + [((rows, depth), f32)] * (not last),
        )
        if raw:
            voxel_raw = raw[0]
        betas.append(beta)
        gathered.append(exchanged(copies, "row"))
        operand, other, squares = call(
            forward_kernel,
            (core_arg, matrix, gathered[-1]),
            [((voxels, depth), bf16), ((half + META, depth), i16), norm_row],
            [((half, depth), f32)],
            scalars=1,
        )
        others = swapped(other)
        (own,) = call(own_kernel, (core_arg, matrix, operand), [((half, depth), f32)], scalars=1)
        (sent,) = call(
            pair_kernel, (own, squares, others), [((peers_xy, share + META, depth), i16)]
        )
        received = exchanged(sent, XY)
        outs = [norm_row, norm_row]
        if not last:
            outs = [((peers_xy, share + META, depth), bf16), ((share, depth), f32), norm_row]
        results = call(
            lambda *refs, last=last: ray_kernel(*refs, last=last), (received, ray_raw, beta), outs
        )
        alphas.append(results[-1])
        if not last:
            copies, ray_raw = results[:2]
            own_rays = exchanged(copies, XY)
            other_rays = swapped(own_rays)
            sums, own_squares = call(
                own_backward_kernel,
                (core_arg, matrix, own_rays),
                [((depth, voxels), f32), norm_row],
                [((half, depth), bf16)],
                scalars=1,
            )
            (sent,) = call(
                backward_kernel,
                (core_arg, matrix, sums, own_squares, other_rays),
                [row_block],
                [((half, depth), bf16), part],
                scalars=1,
            )
    holders = lax.axis_size(ROW_XY)
    squares = results[0] + swapped(results[0])
    squares = exchanged(jnp.broadcast_to(squares[None], (holders, 1, depth)), ROW_XY)
    betas.append(jnp.sqrt(jnp.sum(squares, axis=0) + EPSILON))
    answer, phi_bar = call(
        last_kernel, (*gathered, *alphas, *betas), [((voxels, depth), f32), norm_row]
    )
    return answer, phi_bar[0]


def solution(mesh):
    split = Mesh(mesh.devices.reshape(mesh.shape["row"], 4, 4, 2), ("row", *COL))
    placed = (
        P("row", COL, None, None, None),
        P("row", COL, None),
        P("row", COL, None),
        P("row", COL),
        P("row", None),
    )
    return jax.shard_map(
        body, mesh=split, in_specs=placed, out_specs=(P(COL, None), P()), check_vma=False
    )
```

```python
import jax
import jax.numpy as jnp
from jax import lax
from jax.experimental import pallas as pl
from jax.experimental.pallas import tpu as pltpu
from jax.sharding import Mesh
from jax.sharding import PartitionSpec as P

TILE = 128
WIDTH = 256
CHUNKS = 4
ITERS = 3
EPSILON = 1e-06
XY = ("col_0", "col_1")
COL = ("col_0", "col_1", "col_2")
ROW_XY = ("row", "col_0", "col_1")
STEPS = 32440.0
META = 8
STAGGER = 4500

f32 = jnp.float32
bf16 = jnp.bfloat16
i16 = jnp.int16


def exponent_of(largest):
    return jnp.ceil(jnp.log2(jnp.maximum(largest, 1e-30)))


def coded(array, exponent):
    return jnp.round(array * (jnp.exp2(-exponent) * STEPS)).astype(i16)


def step_of(exponent):
    return jnp.exp2(exponent) * (1.0 / STEPS)


def meta_rows(exponent, squares):
    power = exponent_of(squares)
    scaled = squares * jnp.exp2(-power) * 16384.0
    first = jnp.floor(scaled)
    second = jnp.round((scaled - first) * 16384.0)
    blank = jnp.zeros((META - 4, squares.shape[1]), f32)
    return jnp.concatenate([exponent, power, first, second, blank], axis=0).astype(i16)


def squares_in(meta):
    return jnp.exp2(meta[1:2]) * (meta[2:3] + meta[3:4] * (1.0 / 16384.0)) * (1.0 / 16384.0)


def three_pieces(squares):
    high = squares.astype(bf16)
    rest = squares - high.astype(f32)
    middle = rest.astype(bf16)
    low = (rest - middle.astype(f32)).astype(bf16)
    blank = jnp.zeros((META - 3, squares.shape[1]), f32)
    return jnp.concatenate(
        [high.astype(f32), middle.astype(f32), low.astype(f32), blank], axis=0
    ).astype(bf16)


def column_squares(array):
    return jnp.sum(array * array, axis=0, keepdims=True)


def send_parts(part_ref, out_ref, squares):
    part = part_ref[...]
    exponent = exponent_of(jnp.max(jnp.abs(part), axis=0, keepdims=True))
    meta = meta_rows(exponent, squares)
    peers = out_ref.shape[0]
    rows = part.shape[0] // peers
    codes = coded(part, exponent)
    for peer in range(peers):
        out_ref[peer, :rows, :] = codes[peer * rows : (peer + 1) * rows]
        out_ref[peer, rows : rows + META, :] = meta


def transposed(rays):
    return rays.astype(f32).T.astype(bf16)


def first_kernel(
    start_ref, count_ref, rows_ref, cols_ref, tiles_ref, sinogram_ref,
    matrix_ref, out_ref, share_ref,
    rows_here, cols_here, sinogram_here, tiles_here, rays_ref, part_ref, sems,
):
    copies = [
        pltpu.make_async_copy(rows_ref.at[0, 0], rows_here, sems.at[0]),
        pltpu.make_async_copy(cols_ref.at[0, 0], cols_here, sems.at[1]),
        pltpu.make_async_copy(sinogram_ref, sinogram_here, sems.at[2]),
    ]
    chunk = tiles_here.shape[0] // CHUNKS
    for index in range(CHUNKS):
        slots = pl.ds(index * chunk, chunk)
        source = tiles_ref.at[0, 0, slots]
        copies.append(pltpu.make_async_copy(source, tiles_here.at[slots], sems.at[3 + index]))
    for copy in copies:
        copy.start()
    matrix_ref[...] = jnp.zeros(matrix_ref.shape, bf16)
    for copy in copies[:3]:
        copy.wait()
    sinogram = sinogram_here[...]
    squares = column_squares(sinogram)
    rays_ref[...] = transposed(sinogram.astype(bf16))
    share = share_ref.shape[0]
    share_ref[...] = sinogram_here[pl.ds(pl.multiple_of(start_ref[0], share), share), :]

    def place(slot, carry):
        row = pl.multiple_of(rows_here[slot] * TILE, TILE)
        col = pl.multiple_of(cols_here[slot] * TILE, TILE)
        matrix_ref[pl.ds(row, TILE), pl.ds(col, TILE)] = tiles_here[slot]
        return carry

    for index in range(CHUNKS):
        copies[3 + index].wait()
        end = jnp.minimum(count_ref[0], (index + 1) * chunk)
        lax.fori_loop(index * chunk, end, place, 0)
    rays_t = rays_ref[...]
    for first in range(0, matrix_ref.shape[1], WIDTH):
        part = jnp.dot(rays_t, matrix_ref[:, first : first + WIDTH], preferred_element_type=f32)
        part_ref[first : first + WIDTH, :] = part.T
    send_parts(part_ref, out_ref, squares)

    @pl.when(start_ref[0] < sinogram.shape[0] // 2)
    def _():
        pl.delay(STAGGER)


def half_of_rays(source_ref, rays_ref):
    peers = source_ref.shape[0]
    share = source_ref.shape[1] - META
    squares = jnp.zeros((1, source_ref.shape[2]), f32)
    for peer in range(peers):
        rays_ref[peer * share : (peer + 1) * share, :] = source_ref[peer, :share, :]
        meta = source_ref[peer, share : share + META, :].astype(f32)
        squares = squares + (meta[0:1] + meta[1:2] + meta[2:3])
    return transposed(rays_ref[...]), squares


def half_of_matrix(matrix_ref, which, first):
    half = matrix_ref.shape[0] // 2
    start = pl.multiple_of(which * half, half)
    return matrix_ref[pl.ds(start, half), first : first + WIDTH]


def own_backward_kernel(core_ref, matrix_ref, own_ref, sum_ref, squares_ref, rays_ref):
    rays_t, squares_ref[...] = half_of_rays(own_ref, rays_ref)
    for first in range(0, matrix_ref.shape[1], WIDTH):
        sum_ref[:, first : first + WIDTH] = jnp.dot(
            rays_t, half_of_matrix(matrix_ref, core_ref[0], first), preferred_element_type=f32
        )


def backward_kernel(core_ref, matrix_ref, sum_ref, squares_ref, other_ref, out_ref, rays_ref, part_ref):
    rays_t, squares = half_of_rays(other_ref, rays_ref)
    for first in range(0, matrix_ref.shape[1], WIDTH):
        part = sum_ref[:, first : first + WIDTH] + jnp.dot(
            rays_t, half_of_matrix(matrix_ref, 1 - core_ref[0], first), preferred_element_type=f32
        )
        part_ref[first : first + WIDTH, :] = part.T
    send_parts(part_ref, out_ref, squares_ref[...] + squares)

    @pl.when(core_ref[0] == 0)
    def _():
        pl.delay(STAGGER)


def voxel_kernel(*refs, first):
    if first:
        part_ref, out_ref, beta_ref, *raw_refs = refs
    else:
        part_ref, raw_before_ref, alpha_ref, out_ref, beta_ref, *raw_refs = refs
    peers = part_ref.shape[0]
    rows = part_ref.shape[1] - META
    total = jnp.zeros((rows, part_ref.shape[2]), f32)
    squares = jnp.zeros((1, part_ref.shape[2]), f32)
    for peer in range(peers):
        meta = part_ref[peer, rows : rows + META, :].astype(f32)
        total = total + part_ref[peer, :rows, :].astype(f32) * step_of(meta[0:1])
        squares = squares + squares_in(meta)
    beta = jnp.sqrt(squares + EPSILON)
    raw = total / beta
    if not first:
        raw = raw - beta * (raw_before_ref[...] / alpha_ref[...])
    exponent = exponent_of(jnp.max(jnp.abs(raw), axis=0, keepdims=True))
    codes = coded(raw, exponent)
    meta = meta_rows(exponent, column_squares(raw))
    for peer in range(peers):
        out_ref[peer, :rows, :] = codes
        out_ref[peer, rows : rows + META, :] = meta
    for raw_ref in raw_refs:
        raw_ref[...] = raw
    beta_ref[...] = beta


def dense_rows(matrix_ref, start, operand_ref, put):
    height = 256
    for first in range(0, matrix_ref.shape[0] // 2, height):
        rows = pl.ds(pl.multiple_of(start + first, height), height)
        put(first, jnp.dot(matrix_ref[rows, :], operand_ref[...], preferred_element_type=f32))


def forward_kernel(core_ref, matrix_ref, voxels_ref, operand_ref, other_ref, squares_ref, part_ref):
    peers = voxels_ref.shape[0]
    rows = voxels_ref.shape[1] - META
    squares = jnp.zeros((1, voxels_ref.shape[2]), f32)
    for peer in range(peers):
        meta = voxels_ref[peer, rows : rows + META, :].astype(f32)
        voxels = voxels_ref[peer, :rows, :].astype(f32) * step_of(meta[0:1])
        operand_ref[peer * rows : (peer + 1) * rows, :] = voxels.astype(bf16)
        squares = squares + squares_in(meta)
    half = part_ref.shape[0]

    def put(first, part):
        part_ref[first : first + part.shape[0], :] = part

    dense_rows(matrix_ref, (1 - core_ref[0]) * half, operand_ref, put)
    other = part_ref[...]
    exponent = exponent_of(jnp.max(jnp.abs(other), axis=0, keepdims=True))
    meta = meta_rows(exponent, squares)
    other_ref[:half, :] = coded(other, exponent)
    other_ref[half : half + META, :] = meta
    squares_ref[...] = squares_in(meta.astype(f32))


def own_kernel(core_ref, matrix_ref, operand_ref, own_ref):
    def put(first, part):
        own_ref[first : first + part.shape[0], :] = part

    dense_rows(matrix_ref, core_ref[0] * own_ref.shape[0], operand_ref, put)


def pair_kernel(own_ref, squares_ref, received_ref, out_ref):
    half = own_ref.shape[0]
    peers = out_ref.shape[0]
    share = half // peers
    meta = received_ref[half : half + META, :].astype(f32)
    part = own_ref[...] + received_ref[:half, :].astype(f32) * step_of(meta[0:1])
    squares = squares_ref[...] + squares_in(meta)
    exponent = exponent_of(jnp.max(jnp.abs(part), axis=0, keepdims=True))
    codes = coded(part, exponent)
    meta = meta_rows(exponent, squares)
    for peer in range(peers):
        out_ref[peer, :share, :] = codes[peer * share : (peer + 1) * share]
        out_ref[peer, share : share + META, :] = meta


def ray_kernel(part_ref, ray_before_ref, beta_ref, *out_refs, last):
    peers = part_ref.shape[0]
    share = part_ref.shape[1] - META
    total = jnp.zeros((share, part_ref.shape[2]), f32)
    squares = jnp.zeros((1, part_ref.shape[2]), f32)
    for peer in range(peers):
        meta = part_ref[peer, share : share + META, :].astype(f32)
        total = total + part_ref[peer, :share, :].astype(f32) * step_of(meta[0:1])
        squares = squares + squares_in(meta)
    alpha = jnp.sqrt(squares + EPSILON)
    raw = total / alpha - alpha * (ray_before_ref[...] / beta_ref[...])
    if last:
        squares_ref, alpha_ref = out_refs
        squares_ref[...] = column_squares(raw)
    else:
        out_ref, raw_ref, alpha_ref = out_refs
        pieces = three_pieces(column_squares(raw))
        rounded = raw.astype(bf16)
        for peer in range(peers):
            out_ref[peer, :share, :] = rounded
            out_ref[peer, share : share + META, :] = pieces
        raw_ref[...] = raw
    alpha_ref[...] = alpha


def rotation(rho_bar, beta_norm, phi_bar):
    rho_value = jnp.sqrt(rho_bar * rho_bar + beta_norm * beta_norm)
    cosine = rho_bar / rho_value
    sine_value = beta_norm / rho_value
    return (rho_value, cosine, sine_value, cosine * phi_bar, sine_value * phi_bar)


def last_kernel(voxels0, voxels1, voxels2, alpha0, alpha1, alpha2, beta0, beta1, beta2, beta3, out_ref, phi_ref):
    voxels = (voxels0, voxels1, voxels2)
    alphas = [ref[...] for ref in (alpha0, alpha1, alpha2)]
    betas = [ref[...] for ref in (beta0, beta1, beta2, beta3)]
    phi_bar = betas[0]
    rho_bar = alphas[0]
    steps, turns = [], []
    for step in range(ITERS):
        rho_value, cosine, sine_value, phi_value, phi_bar = rotation(rho_bar, betas[step + 1], phi_bar)
        steps.append(phi_value / rho_value)
        if step + 1 < ITERS:
            turns.append(sine_value * alphas[step + 1] / rho_value)
            rho_bar = -cosine * alphas[step + 1]
    peers = voxels0.shape[0]
    rows = voxels0.shape[1] - META
    for peer in range(peers):
        solution_rows = search_dir = None
        for step in range(ITERS):
            meta = voxels[step][peer, rows : rows + META, :].astype(f32)
            raw = voxels[step][peer, :rows, :].astype(f32) * step_of(meta[0:1])
            voxel_vec = raw / alphas[step]
            if step == 0:
                search_dir = voxel_vec
                solution_rows = steps[0] * search_dir
            else:
                search_dir = voxel_vec - turns[step - 1] * search_dir
                solution_rows = solution_rows + steps[step] * search_dir
        out_ref[peer * rows : (peer + 1) * rows, :] = solution_rows
    phi_ref[...] = phi_bar


def whole(memory=pltpu.VMEM):
    return pl.BlockSpec(memory_space=memory)


def call(kernel, operands, outs, scratch=(), scalars=0, limit=8):
    shapes = [jax.ShapeDtypeStruct(shape, dtype) for shape, dtype in outs]
    return pl.pallas_call(
        kernel,
        in_specs=[whole(pltpu.SMEM)] * scalars + [whole()] * (len(operands) - scalars),
        out_specs=[whole()] * len(outs),
        out_shape=shapes,
        scratch_shapes=[pltpu.VMEM(shape, dtype) for shape, dtype in scratch],
        compiler_params=pltpu.CompilerParams(vmem_limit_bytes=limit * 1024 * 1024),
    )(*operands)


def exchanged(array, axis):
    return lax.all_to_all(array, axis, 0, 0, tiled=True)


def body(tile_values, tile_rows, tile_cols, tile_count, sinogram):
    rays, depth = sinogram.shape
    peers_row = lax.axis_size("row")
    peers_xy = lax.axis_size(XY)
    voxels = rays
    rows = voxels // peers_row
    half = rays // 2
    share = half // peers_xy
    core = lax.axis_index("col_2")
    core_arg = core.astype(jnp.int32).reshape(1)

    def swapped(array):
        return lax.ppermute(array, "col_2", [(0, 1), (1, 0)])

    row_block = ((peers_row, rows + META, depth), i16)
    norm_row = ((1, depth), f32)
    part = ((rays, depth), f32)

    start = (core * half + lax.axis_index(XY) * share).astype(jnp.int32).reshape(1)
    slots = tile_rows.shape[-1]
    matrix, sent, ray_raw = pl.pallas_call(
        first_kernel,
        in_specs=[whole(pltpu.SMEM)] * 2 + [whole(pltpu.HBM)] * 4,
        out_specs=[whole()] * 3,
        out_shape=[
            jax.ShapeDtypeStruct((rays, voxels), bf16),
            jax.ShapeDtypeStruct(*row_block),
            jax.ShapeDtypeStruct((share, depth), f32),
        ],
        scratch_shapes=[
            pltpu.SMEM((slots,), jnp.int32),
            pltpu.SMEM((slots,), jnp.int32),
            pltpu.VMEM((rays, depth), f32),
            pltpu.VMEM(tile_values.shape[2:], bf16),
            pltpu.VMEM((depth, rays), bf16),
            pltpu.VMEM((rays, depth), f32),
            pltpu.SemaphoreType.DMA((3 + CHUNKS,)),
        ],
        compiler_params=pltpu.CompilerParams(vmem_limit_bytes=16 * 1024 * 1024),
    )(
        start,
        tile_count[0],
        *(
            pltpu.with_memory_space_constraint(array, pltpu.HBM)
            for array in (tile_rows, tile_cols, tile_values, sinogram)
        ),
    )
    voxel_raw = None
    alphas, betas, gathered = [], [], []
    for step in range(ITERS):
        received = exchanged(sent, "row")
        before = () if step == 0 else (voxel_raw, alphas[-1])
        last = step + 1 == ITERS
        copies, beta, *raw = call(
            lambda *refs, first=step == 0: voxel_kernel(*refs, first=first),
            (received, *before),
            [row_block, norm_row] + [((rows, depth), f32)] * (not last),
        )
        if raw:
            voxel_raw = raw[0]
        betas.append(beta)
        gathered.append(exchanged(copies, "row"))
        operand, other, squares = call(
            forward_kernel,
            (core_arg, matrix, gathered[-1]),
            [((voxels, depth), bf16), ((half + META, depth), i16), norm_row],
            [((half, depth), f32)],
            scalars=1,
        )
        others = swapped(other)
        (own,) = call(own_kernel, (core_arg, matrix, operand), [((half, depth), f32)], scalars=1)
        (sent,) = call(
            pair_kernel, (own, squares, others), [((peers_xy, share + META, depth), i16)]
        )
        received = exchanged(sent, XY)
        outs = [norm_row, norm_row]
        if not last:
            outs = [((peers_xy, share + META, depth), bf16), ((share, depth), f32), norm_row]
        results = call(
            lambda *refs, last=last: ray_kernel(*refs, last=last), (received, ray_raw, beta), outs
        )
        alphas.append(results[-1])
        if not last:
            copies, ray_raw = results[:2]
            own_rays = exchanged(copies, XY)
            other_rays = swapped(own_rays)
            sums, own_squares = call(
                own_backward_kernel,
                (core_arg, matrix, own_rays),
                [((depth, voxels), f32), norm_row],
                [((half, depth), bf16)],
                scalars=1,
            )
            (sent,) = call(
                backward_kernel,
                (core_arg, matrix, sums, own_squares, other_rays),
                [row_block],
                [((half, depth), bf16), part],
                scalars=1,
            )
    holders = lax.axis_size(ROW_XY)
    squares = results[0] + swapped(results[0])
    squares = exchanged(jnp.broadcast_to(squares[None], (holders, 1, depth)), ROW_XY)
    betas.append(jnp.sqrt(jnp.sum(squares, axis=0) + EPSILON))
    answer, phi_bar = call(
        last_kernel, (*gathered, *alphas, *betas), [((voxels, depth), f32), norm_row]
    )
    return answer, phi_bar[0]


def solution(mesh):
    split = Mesh(mesh.devices.reshape(mesh.shape["row"], 4, 4, 2), ("row", *COL))
    placed = (
        P("row", COL, None, None, None),
        P("row", COL, None),
        P("row", COL, None),
        P("row", COL),
        P("row", None),
    )
    return jax.shard_map(
        body, mesh=split, in_specs=placed, out_specs=(P(COL, None), P()), check_vma=False
    )
```

```python
import jax
import jax.numpy as jnp
from jax import lax
from jax.experimental import pallas as pl
from jax.experimental.pallas import tpu as pltpu
from jax.sharding import Mesh
from jax.sharding import PartitionSpec as P

TILE = 128
WIDTH = 512
CHUNKS = 4
ITERS = 3
EPSILON = 1e-06
XY = ("col_0", "col_1")
COL = ("col_0", "col_1", "col_2")
ROW_XY = ("row", "col_0", "col_1")
STEPS = 32440.0
META = 8
STAGGER = 4500

f32 = jnp.float32
bf16 = jnp.bfloat16
i16 = jnp.int16


def exponent_of(largest):
    return jnp.ceil(jnp.log2(jnp.maximum(largest, 1e-30)))


def coded(array, exponent):
    return jnp.round(array * (jnp.exp2(-exponent) * STEPS)).astype(i16)


def step_of(exponent):
    return jnp.exp2(exponent) * (1.0 / STEPS)


def meta_rows(exponent, squares):
    power = exponent_of(squares)
    scaled = squares * jnp.exp2(-power) * 16384.0
    first = jnp.floor(scaled)
    second = jnp.round((scaled - first) * 16384.0)
    blank = jnp.zeros((META - 4, squares.shape[1]), f32)
    return jnp.concatenate([exponent, power, first, second, blank], axis=0).astype(i16)


def squares_in(meta):
    return jnp.exp2(meta[1:2]) * (meta[2:3] + meta[3:4] * (1.0 / 16384.0)) * (1.0 / 16384.0)


def three_pieces(squares):
    high = squares.astype(bf16)
    rest = squares - high.astype(f32)
    middle = rest.astype(bf16)
    low = (rest - middle.astype(f32)).astype(bf16)
    blank = jnp.zeros((META - 3, squares.shape[1]), f32)
    return jnp.concatenate(
        [high.astype(f32), middle.astype(f32), low.astype(f32), blank], axis=0
    ).astype(bf16)


def column_squares(array):
    return jnp.sum(array * array, axis=0, keepdims=True)


def send_parts(part_ref, out_ref, squares):
    part = part_ref[...]
    exponent = exponent_of(jnp.max(jnp.abs(part), axis=0, keepdims=True))
    meta = meta_rows(exponent, squares)
    peers = out_ref.shape[0]
    rows = part.shape[0] // peers
    codes = coded(part, exponent)
    for peer in range(peers):
        out_ref[peer, :rows, :] = codes[peer * rows : (peer + 1) * rows]
        out_ref[peer, rows : rows + META, :] = meta


def transposed(rays):
    return rays.astype(f32).T.astype(bf16)


def first_kernel(
    start_ref, count_ref, rows_ref, cols_ref, tiles_ref, sinogram_ref,
    matrix_ref, out_ref, share_ref,
    rows_here, cols_here, sinogram_here, tiles_here, rays_ref, part_ref, sems,
):
    copies = [
        pltpu.make_async_copy(rows_ref.at[0, 0], rows_here, sems.at[0]),
        pltpu.make_async_copy(cols_ref.at[0, 0], cols_here, sems.at[1]),
        pltpu.make_async_copy(sinogram_ref, sinogram_here, sems.at[2]),
    ]
    chunk = tiles_here.shape[0] // CHUNKS
    for index in range(CHUNKS):
        slots = pl.ds(index * chunk, chunk)
        source = tiles_ref.at[0, 0, slots]
        copies.append(pltpu.make_async_copy(source, tiles_here.at[slots], sems.at[3 + index]))
    for copy in copies:
        copy.start()
    matrix_ref[...] = jnp.zeros(matrix_ref.shape, bf16)
    for copy in copies[:3]:
        copy.wait()
    sinogram = sinogram_here[...]
    squares = column_squares(sinogram)
    rays_ref[...] = transposed(sinogram.astype(bf16))
    share = share_ref.shape[0]
    share_ref[...] = sinogram_here[pl.ds(pl.multiple_of(start_ref[0], share), share), :]

    def place(slot, carry):
        row = pl.multiple_of(rows_here[slot] * TILE, TILE)
        col = pl.multiple_of(cols_here[slot] * TILE, TILE)
        matrix_ref[pl.ds(row, TILE), pl.ds(col, TILE)] = tiles_here[slot]
        return carry

    for index in range(CHUNKS):
        copies[3 + index].wait()
        end = jnp.minimum(count_ref[0], (index + 1) * chunk)
        lax.fori_loop(index * chunk, end, place, 0)
    rays_t = rays_ref[...]
    for first in range(0, matrix_ref.shape[1], WIDTH):
        part = jnp.dot(rays_t, matrix_ref[:, first : first + WIDTH], preferred_element_type=f32)
        part_ref[first : first + WIDTH, :] = part.T
    send_parts(part_ref, out_ref, squares)

    @pl.when(start_ref[0] < sinogram.shape[0] // 2)
    def _():
        pl.delay(STAGGER)


def half_of_rays(source_ref, rays_ref):
    peers = source_ref.shape[0]
    share = source_ref.shape[1] - META
    squares = jnp.zeros((1, source_ref.shape[2]), f32)
    for peer in range(peers):
        rays_ref[peer * share : (peer + 1) * share, :] = source_ref[peer, :share, :]
        meta = source_ref[peer, share : share + META, :].astype(f32)
        squares = squares + (meta[0:1] + meta[1:2] + meta[2:3])
    return transposed(rays_ref[...]), squares


def half_of_matrix(matrix_ref, which, first):
    half = matrix_ref.shape[0] // 2
    start = pl.multiple_of(which * half, half)
    return matrix_ref[pl.ds(start, half), first : first + WIDTH]


def own_backward_kernel(core_ref, matrix_ref, own_ref, sum_ref, squares_ref, rays_ref):
    rays_t, squares_ref[...] = half_of_rays(own_ref, rays_ref)
    for first in range(0, matrix_ref.shape[1], WIDTH):
        sum_ref[:, first : first + WIDTH] = jnp.dot(
            rays_t, half_of_matrix(matrix_ref, core_ref[0], first), preferred_element_type=f32
        )


def backward_kernel(core_ref, matrix_ref, sum_ref, squares_ref, other_ref, out_ref, rays_ref, part_ref):
    rays_t, squares = half_of_rays(other_ref, rays_ref)
    for first in range(0, matrix_ref.shape[1], WIDTH):
        part = sum_ref[:, first : first + WIDTH] + jnp.dot(
            rays_t, half_of_matrix(matrix_ref, 1 - core_ref[0], first), preferred_element_type=f32
        )
        part_ref[first : first + WIDTH, :] = part.T
    send_parts(part_ref, out_ref, squares_ref[...] + squares)

    @pl.when(core_ref[0] == 0)
    def _():
        pl.delay(STAGGER)


def voxel_kernel(*refs, first):
    if first:
        part_ref, out_ref, beta_ref, *raw_refs = refs
    else:
        part_ref, raw_before_ref, alpha_ref, out_ref, beta_ref, *raw_refs = refs
    peers = part_ref.shape[0]
    rows = part_ref.shape[1] - META
    total = jnp.zeros((rows, part_ref.shape[2]), f32)
    squares = jnp.zeros((1, part_ref.shape[2]), f32)
    for peer in range(peers):
        meta = part_ref[peer, rows : rows + META, :].astype(f32)
        total = total + part_ref[peer, :rows, :].astype(f32) * step_of(meta[0:1])
        squares = squares + squares_in(meta)
    beta = jnp.sqrt(squares + EPSILON)
    raw = total / beta
    if not first:
        raw = raw - beta * (raw_before_ref[...] / alpha_ref[...])
    exponent = exponent_of(jnp.max(jnp.abs(raw), axis=0, keepdims=True))
    codes = coded(raw, exponent)
    meta = meta_rows(exponent, column_squares(raw))
    for peer in range(peers):
        out_ref[peer, :rows, :] = codes
        out_ref[peer, rows : rows + META, :] = meta
    for raw_ref in raw_refs:
        raw_ref[...] = raw
    beta_ref[...] = beta


def dense_rows(matrix_ref, start, operand_ref, put):
    height = 256
    for first in range(0, matrix_ref.shape[0] // 2, height):
        rows = pl.ds(pl.multiple_of(start + first, height), height)
        put(first, jnp.dot(matrix_ref[rows, :], operand_ref[...], preferred_element_type=f32))


def forward_kernel(core_ref, matrix_ref, voxels_ref, operand_ref, other_ref, squares_ref, part_ref):
    peers = voxels_ref.shape[0]
    rows = voxels_ref.shape[1] - META
    squares = jnp.zeros((1, voxels_ref.shape[2]), f32)
    for peer in range(peers):
        meta = voxels_ref[peer, rows : rows + META, :].astype(f32)
        voxels = voxels_ref[peer, :rows, :].astype(f32) * step_of(meta[0:1])
        operand_ref[peer * rows : (peer + 1) * rows, :] = voxels.astype(bf16)
        squares = squares + squares_in(meta)
    half = part_ref.shape[0]

    def put(first, part):
        part_ref[first : first + part.shape[0], :] = part

    dense_rows(matrix_ref, (1 - core_ref[0]) * half, operand_ref, put)
    other = part_ref[...]
    exponent = exponent_of(jnp.max(jnp.abs(other), axis=0, keepdims=True))
    meta = meta_rows(exponent, squares)
    other_ref[:half, :] = coded(other, exponent)
    other_ref[half : half + META, :] = meta
    squares_ref[...] = squares_in(meta.astype(f32))


def own_kernel(core_ref, matrix_ref, operand_ref, own_ref):
    def put(first, part):
        own_ref[first : first + part.shape[0], :] = part

    dense_rows(matrix_ref, core_ref[0] * own_ref.shape[0], operand_ref, put)


def pair_kernel(own_ref, squares_ref, received_ref, out_ref):
    half = own_ref.shape[0]
    peers = out_ref.shape[0]
    share = half // peers
    meta = received_ref[half : half + META, :].astype(f32)
    part = own_ref[...] + received_ref[:half, :].astype(f32) * step_of(meta[0:1])
    squares = squares_ref[...] + squares_in(meta)
    exponent = exponent_of(jnp.max(jnp.abs(part), axis=0, keepdims=True))
    codes = coded(part, exponent)
    meta = meta_rows(exponent, squares)
    for peer in range(peers):
        out_ref[peer, :share, :] = codes[peer * share : (peer + 1) * share]
        out_ref[peer, share : share + META, :] = meta


def ray_kernel(part_ref, ray_before_ref, beta_ref, *out_refs, last):
    peers = part_ref.shape[0]
    share = part_ref.shape[1] - META
    total = jnp.zeros((share, part_ref.shape[2]), f32)
    squares = jnp.zeros((1, part_ref.shape[2]), f32)
    for peer in range(peers):
        meta = part_ref[peer, share : share + META, :].astype(f32)
        total = total + part_ref[peer, :share, :].astype(f32) * step_of(meta[0:1])
        squares = squares + squares_in(meta)
    alpha = jnp.sqrt(squares + EPSILON)
    raw = total / alpha - alpha * (ray_before_ref[...] / beta_ref[...])
    if last:
        squares_ref, alpha_ref = out_refs
        squares_ref[...] = column_squares(raw)
    else:
        out_ref, raw_ref, alpha_ref = out_refs
        pieces = three_pieces(column_squares(raw))
        rounded = raw.astype(bf16)
        for peer in range(peers):
            out_ref[peer, :share, :] = rounded
            out_ref[peer, share : share + META, :] = pieces
        raw_ref[...] = raw
    alpha_ref[...] = alpha


def rotation(rho_bar, beta_norm, phi_bar):
    rho_value = jnp.sqrt(rho_bar * rho_bar + beta_norm * beta_norm)
    cosine = rho_bar / rho_value
    sine_value = beta_norm / rho_value
    return (rho_value, cosine, sine_value, cosine * phi_bar, sine_value * phi_bar)


def last_kernel(voxels0, voxels1, voxels2, alpha0, alpha1, alpha2, beta0, beta1, beta2, beta3, out_ref, phi_ref):
    voxels = (voxels0, voxels1, voxels2)
    alphas = [ref[...] for ref in (alpha0, alpha1, alpha2)]
    betas = [ref[...] for ref in (beta0, beta1, beta2, beta3)]
    phi_bar = betas[0]
    rho_bar = alphas[0]
    steps, turns = [], []
    for step in range(ITERS):
        rho_value, cosine, sine_value, phi_value, phi_bar = rotation(rho_bar, betas[step + 1], phi_bar)
        steps.append(phi_value / rho_value)
        if step + 1 < ITERS:
            turns.append(sine_value * alphas[step + 1] / rho_value)
            rho_bar = -cosine * alphas[step + 1]
    peers = voxels0.shape[0]
    rows = voxels0.shape[1] - META
    for peer in range(peers):
        solution_rows = search_dir = None
        for step in range(ITERS):
            meta = voxels[step][peer, rows : rows + META, :].astype(f32)
            raw = voxels[step][peer, :rows, :].astype(f32) * step_of(meta[0:1])
            voxel_vec = raw / alphas[step]
            if step == 0:
                search_dir = voxel_vec
                solution_rows = steps[0] * search_dir
            else:
                search_dir = voxel_vec - turns[step - 1] * search_dir
                solution_rows = solution_rows + steps[step] * search_dir
        out_ref[peer * rows : (peer + 1) * rows, :] = solution_rows
    phi_ref[...] = phi_bar


def whole(memory=pltpu.VMEM):
    return pl.BlockSpec(memory_space=memory)


def call(kernel, operands, outs, scratch=(), scalars=0, limit=8):
    shapes = [jax.ShapeDtypeStruct(shape, dtype) for shape, dtype in outs]
    return pl.pallas_call(
        kernel,
        in_specs=[whole(pltpu.SMEM)] * scalars + [whole()] * (len(operands) - scalars),
        out_specs=[whole()] * len(outs),
        out_shape=shapes,
        scratch_shapes=[pltpu.VMEM(shape, dtype) for shape, dtype in scratch],
        compiler_params=pltpu.CompilerParams(vmem_limit_bytes=limit * 1024 * 1024),
    )(*operands)


def exchanged(array, axis):
    return lax.all_to_all(array, axis, 0, 0, tiled=True)


def body(tile_values, tile_rows, tile_cols, tile_count, sinogram):
    rays, depth = sinogram.shape
    peers_row = lax.axis_size("row")
    peers_xy = lax.axis_size(XY)
    voxels = rays
    rows = voxels // peers_row
    half = rays // 2
    share = half // peers_xy
    core = lax.axis_index("col_2")
    core_arg = core.astype(jnp.int32).reshape(1)

    def swapped(array):
        return lax.ppermute(array, "col_2", [(0, 1), (1, 0)])

    row_block = ((peers_row, rows + META, depth), i16)
    norm_row = ((1, depth), f32)
    part = ((rays, depth), f32)

    start = (core * half + lax.axis_index(XY) * share).astype(jnp.int32).reshape(1)
    slots = tile_rows.shape[-1]
    matrix, sent, ray_raw = pl.pallas_call(
        first_kernel,
        in_specs=[whole(pltpu.SMEM)] * 2 + [whole(pltpu.HBM)] * 4,
        out_specs=[whole()] * 3,
        out_shape=[
            jax.ShapeDtypeStruct((rays, voxels), bf16),
            jax.ShapeDtypeStruct(*row_block),
            jax.ShapeDtypeStruct((share, depth), f32),
        ],
        scratch_shapes=[
            pltpu.SMEM((slots,), jnp.int32),
            pltpu.SMEM((slots,), jnp.int32),
            pltpu.VMEM((rays, depth), f32),
            pltpu.VMEM(tile_values.shape[2:], bf16),
            pltpu.VMEM((depth, rays), bf16),
            pltpu.VMEM((rays, depth), f32),
            pltpu.SemaphoreType.DMA((3 + CHUNKS,)),
        ],
        compiler_params=pltpu.CompilerParams(vmem_limit_bytes=16 * 1024 * 1024),
    )(
        start,
        tile_count[0],
        *(
            pltpu.with_memory_space_constraint(array, pltpu.HBM)
            for array in (tile_rows, tile_cols, tile_values, sinogram)
        ),
    )
    voxel_raw = None
    alphas, betas, gathered = [], [], []
    for step in range(ITERS):
        received = exchanged(sent, "row")
        before = () if step == 0 else (voxel_raw, alphas[-1])
        last = step + 1 == ITERS
        copies, beta, *raw = call(
            lambda *refs, first=step == 0: voxel_kernel(*refs, first=first),
            (received, *before),
            [row_block, norm_row] + [((rows, depth), f32)] * (not last),
        )
        if raw:
            voxel_raw = raw[0]
        betas.append(beta)
        gathered.append(exchanged(copies, "row"))
        operand, other, squares = call(
            forward_kernel,
            (core_arg, matrix, gathered[-1]),
            [((voxels, depth), bf16), ((half + META, depth), i16), norm_row],
            [((half, depth), f32)],
            scalars=1,
        )
        others = swapped(other)
        (own,) = call(own_kernel, (core_arg, matrix, operand), [((half, depth), f32)], scalars=1)
        (sent,) = call(
            pair_kernel, (own, squares, others), [((peers_xy, share + META, depth), i16)]
        )
        received = exchanged(sent, XY)
        outs = [norm_row, norm_row]
        if not last:
            outs = [((peers_xy, share + META, depth), bf16), ((share, depth), f32), norm_row]
        results = call(
            lambda *refs, last=last: ray_kernel(*refs, last=last), (received, ray_raw, beta), outs
        )
        alphas.append(results[-1])
        if not last:
            copies, ray_raw = results[:2]
            own_rays = exchanged(copies, XY)
            other_rays = swapped(own_rays)
            sums, own_squares = call(
                own_backward_kernel,
                (core_arg, matrix, own_rays),
                [((depth, voxels), f32), norm_row],
                [((half, depth), bf16)],
                scalars=1,
            )
            (sent,) = call(
                backward_kernel,
                (core_arg, matrix, sums, own_squares, other_rays),
                [row_block],
                [((half, depth), bf16), part],
                scalars=1,
            )
    holders = lax.axis_size(ROW_XY)
    squares = results[0] + swapped(results[0])
    squares = exchanged(jnp.broadcast_to(squares[None], (holders, 1, depth)), ROW_XY)
    betas.append(jnp.sqrt(jnp.sum(squares, axis=0) + EPSILON))
    answer, phi_bar = call(
        last_kernel, (*gathered, *alphas, *betas), [((voxels, depth), f32), norm_row]
    )
    return answer, phi_bar[0]


def solution(mesh):
    split = Mesh(mesh.devices.reshape(mesh.shape["row"], 4, 4, 2), ("row", *COL))
    placed = (
        P("row", COL, None, None, None),
        P("row", COL, None),
        P("row", COL, None),
        P("row", COL),
        P("row", None),
    )
    return jax.shard_map(
        body, mesh=split, in_specs=placed, out_specs=(P(COL, None), P()), check_vma=False
    )
```
